32 devices in a mesh: vocab: 2 (over y), tok: 16 (over z, x, core).
Axes of the slice: x: 2, y: 2, z: 4, core: 2. Of those that a mesh axis runs over, the one named last changes fastest.
Arguments:
- hidden: bfloat16 [2048, 3584], P('tok'), may hold values from -64 to 64
- norm_gain: float32 [3584], replicated, may hold values from 0.1 to 1.9
- unembed: bfloat16 [3584, 152064], P(None, ('vocab', 'tok')), may hold values from -1 to 1
- target_ids: int32 [2048], replicated, may hold values from 0 to 152063
- loss_mask: int32 [2048], P(('vocab', 'tok')), may hold values 0 or 1
- seq_ids: int32 [2048], P(('vocab', 'tok')), may hold values from 0 to 3, never falling along the last dimension, each value on 1 to 1024 neighbouring positions
- advantages: float32 [2048], P(('vocab', 'tok')), may hold values from -20 to 20
- prox_logp: float32 [2048], P(('vocab', 'tok')), may hold values from -22 to -10
- behav_logp: float32 [2048], P(('vocab', 'tok')), may hold values from -22 to -10
Outputs:
- logp: float32 [2048], P(('vocab', 'tok'))
- token_loss: float32 [2048], P(('vocab', 'tok'))
- policy_loss: float32 [], replicated
- seq_means: float32 [2, 4], replicated
The draws below stay inside these ranges and needn't reach their ends.
All inputs are finite; a program needn't handle non-finite values. No bound on the sum of `loss_mask` on one device may be relied on, other than what follows from the above.
Results may differ from the reference program's by a relative error of at most 0.0035.
Values may be sent and summed in bfloat16 or wider, within the bound.
A program may use at most 128 MiB of HBM per device.

```python
import math
import jax
import jax.numpy as jnp
import numpy as np
from jax import lax

D = 3584
V = 152064
LENGTH = 512
TOKENS = 2048
SEQS = 4
N_VOCAB = 2
N_TOK = 16


def paired_draw(key):
    base = jax.random.fold_in(key, 11)
    key_hidden, key_weight = jax.random.split(base, 2)
    values = jnp.clip(jax.random.normal(key_hidden, (TOKENS, D), jnp.float32), -6.0, 6.0)
    weight = jnp.clip(jax.random.normal(key_weight, (D, V), jnp.float32), -6.0, 6.0) * (3.0 / jnp.sqrt(jnp.float32(D)))
    return (values, weight)


def draw_hidden(key, part):
    values, weight = paired_draw(key)
    return values.astype(jnp.bfloat16)


def draw_unembed(key, part):
    values, weight = paired_draw(key)
    return weight.astype(jnp.bfloat16)


def draw_advantages(key, part):
    base = jax.random.fold_in(key, 23)
    ramp = 1.0 + 2.0 * jnp.arange(TOKENS, dtype=jnp.float32) / (TOKENS - 1)
    noise = jnp.clip(jax.random.normal(base, (TOKENS,), jnp.float32), -5.0, 5.0)
    return noise * ramp


def plant(array, key, smallest, high):
    longest = array.shape.index(max(array.shape))
    spots = []
    for shift in (0, 1):
        where = [jax.random.randint(jax.random.fold_in(key, axis), (), 0, length) for axis, length in enumerate(array.shape)]
        where[longest] = (where[longest] + shift) % array.shape[longest]
        spots.append(tuple(where))
    return array.at[spots[0]].set(smallest).at[spots[1]].set(high)


def steps_of(rng, shape, cuts, smallest, top_value):
    def one(position, shards_of):
        heights = jax.random.uniform(jax.random.fold_in(jax.random.fold_in(rng, 6), position), (shards_of,), jnp.float32, smallest / len(cuts), top_value / len(cuts))
        return jnp.repeat(jnp.exp(heights), shape[position] // shards_of).reshape((-1,) + (1,) * (len(shape) - position - 1))

    gain = one(*cuts[0])
    for cut in cuts[1:]:
        gain = gain * one(*cut)
    return gain


def ranked_wide(own_key, dims, number_of, slope):
    weights = [min(1 << octave, number_of + 1 - (1 << octave)) * (1 << 20) // math.isqrt((1 << octave) ** slope) + 1 for octave in range((number_of + 1).bit_length()) if 1 << octave <= number_of]
    spread = 1 + sum(weights) // (1 << 30)
    grid = np.cumsum(np.array([max(1, weight // spread) for weight in weights]))
    pick = jax.random.randint(jax.random.fold_in(own_key, 1), dims, 0, int(grid[len(weights) - 1]))
    start = jnp.left_shift(1, jnp.searchsorted(jnp.asarray(grid, jnp.int32), pick, side="right").astype(jnp.int32))
    rank = start - 1 + jax.random.randint(jax.random.fold_in(own_key, 4), dims, 0, 1 << 30) % jnp.minimum(start, number_of + 1 - start)
    return jax.random.permutation(jax.random.fold_in(own_key, 2), number_of)[rank].astype(jnp.int32)


def length_profile(count, total, reach, slope):
    weights = [(1 << 20) // math.isqrt(grade ** slope) + 1 for grade in range(2, count + 1)]
    rest, holding = total - reach - (count - 1), [1] * (count - 1)
    while rest > 0:
        movable = [i for i in range(count - 1) if holding[i] < reach]
        whole, left = sum([weights[i] for i in movable]), rest
        for i in movable:
            more = min(reach - holding[i], max(1, left * weights[i] // whole), rest)
            holding[i] = holding[i] + more
            rest = rest - more
    return np.array([reach] + holding)


def uneven(stream_key, count, total, reach, skew):
    if count == 2:
        one = jax.random.randint(stream_key, (), max(1, total - reach), min(reach, total - 1) + 1)
        return jnp.stack([one, total - one])
    sizes = jnp.asarray(length_profile(count, total, reach, skew), jnp.int32)
    twos = (count - 1) // 2
    source_of, sink = sizes[1:1 + 2 * twos:2], sizes[2:2 + 2 * twos:2]
    slack = jnp.minimum(source_of - 1, reach - sink)
    passed = jax.random.randint(jax.random.fold_in(stream_key, 1), (twos,), 0, 1 << 20) % (slack + 1)
    sizes = sizes.at[1:1 + 2 * twos:2].set(source_of - passed).at[2:2 + 2 * twos:2].set(sink + passed)
    return sizes[jax.random.permutation(jax.random.fold_in(stream_key, 2), count)]


def setup_inputs(seed: int = 0) -> dict:
    key_list = jax.random.split(jax.random.key(seed), 10)
    return {
        "hidden": draw_hidden(jax.random.fold_in(key_list[9], 71), 0),
        "norm_gain": jnp.clip(1.0 + 0.18 * jax.random.normal(key_list[1], (D,), jnp.float32), 0.1, 1.9),
        "unembed": draw_unembed(jax.random.fold_in(key_list[9], 71), 0),
        "target_ids": plant(ranked_wide(key_list[3], (TOKENS,), V, 2), jax.random.fold_in(key_list[3], 3), 0, V - 1).astype(jnp.int32),
        "loss_mask": plant((jax.random.randint(key_list[4], (TOKENS,), 0, 4) < 3).astype(jnp.int32), jax.random.fold_in(key_list[4], 1), 0, 1),
        "seq_ids": jnp.searchsorted(jnp.cumsum(uneven(key_list[5], SEQS, TOKENS, 2 * LENGTH, 1)), jnp.arange(TOKENS), side="right").astype(jnp.int32),
        "advantages": draw_advantages(jax.random.fold_in(key_list[9], 71), 0),
        "prox_logp": jnp.clip(-22.0 + 12.0 * jax.random.uniform(key_list[7], (TOKENS,), jnp.float32) ** steps_of(key_list[7], (TOKENS,), ((0, 32),), -0.2, 0.2), -22.0, -10.0),
        "behav_logp": jnp.clip(-22.0 + 12.0 * jax.random.uniform(key_list[8], (TOKENS,), jnp.float32) ** steps_of(key_list[8], (TOKENS,), ((0, 32),), -0.2, 0.2), -22.0, -10.0),
    }


def reference(hidden, norm_gain, unembed, target_ids, loss_mask, seq_ids, advantages, prox_logp, behav_logp):
    values = hidden.astype(jnp.float32)
    scale = lax.rsqrt(lax.optimization_barrier(jnp.mean(values * values, axis=1, keepdims=True)) + 1e-06)
    normed = (values * scale * norm_gain).astype(jnp.bfloat16)
    blocks = N_VOCAB * N_TOK
    width = V // blocks

    def step(carry, index):
        peak, total, picked = carry
        start = (index * width).astype(jnp.int32)
        columns = lax.dynamic_slice_in_dim(unembed, start, width, 1)
        logits = jnp.dot(normed, columns, preferred_element_type=jnp.float32)
        top = lax.optimization_barrier(jnp.max(logits, axis=1))
        newpeak = jnp.maximum(peak, top)
        total = total * jnp.exp(peak - newpeak) + lax.optimization_barrier(jnp.sum(jnp.exp(logits - newpeak[:, None]), axis=1))
        cols = lax.broadcasted_iota(jnp.int32, logits.shape, 1)
        hit = cols == (target_ids - start)[:, None]
        picked = picked + lax.optimization_barrier(jnp.sum(jnp.where(hit, logits, jnp.float32(0.0)), axis=1))
        return ((newpeak, total, picked), None)
    init = (jnp.full((TOKENS,), -1e+30, jnp.float32), jnp.zeros((TOKENS,), jnp.float32), jnp.zeros((TOKENS,), jnp.float32))
    (peak, total, picked), _ = lax.scan(step, init, jnp.arange(blocks, dtype=jnp.int32))
    logp = picked - peak - jnp.log(total)
    weight_b = jnp.minimum(jnp.exp(prox_logp - behav_logp), 5.0)
    ratio = jnp.exp(logp - prox_logp)
    surr = jnp.minimum(ratio * advantages, jnp.clip(ratio, 0.8, 1.2) * advantages)
    surr = jnp.where(advantages < 0, jnp.maximum(surr, 3.0 * advantages), surr)
    token_loss = -weight_b * surr
    member = (jnp.arange(SEQS, dtype=jnp.int32)[:, None] == seq_ids[None, :]).astype(jnp.float32)
    member = member * loss_mask.astype(jnp.float32)[None, :]
    loss_sum = lax.optimization_barrier(jnp.sum(member * token_loss[None, :], axis=1))
    diff_sum = lax.optimization_barrier(jnp.sum(member * (logp - prox_logp)[None, :], axis=1))
    count = lax.optimization_barrier(jnp.sum(member, axis=1))
    policy_loss = jnp.sum(loss_sum) / jnp.maximum(jnp.sum(count), 1.0)
    floor = jnp.maximum(count, 1.0)
    seq_means = jnp.stack([loss_sum / floor, diff_sum / floor])
    return (logp, token_loss, policy_loss, seq_means)
```

```python
import jax
import jax.numpy as jnp
from jax import lax
from jax.experimental import pallas as pl
from jax.experimental.pallas import tpu as pltpu
from jax.sharding import PartitionSpec as P

LENGTH = 512
LANES = 128
HALVES = 2
LOW = -1e30
MESH = pl.DeviceIdType.MESH


def sections_of(columns):
    tiles = (columns + 255) // 256
    parts = 3 if tiles >= 3 else 1
    cuts = [tiles * i // parts * 256 for i in range(parts)] + [columns]
    return [(cuts[i], cuts[i + 1] - cuts[i]) for i in range(parts)]


def padded(width):
    return (width + LANES - 1) // LANES * LANES


def pick(index, values):
    found = values[0]
    for k in range(1, len(values)):
        found = jnp.where(index == k, values[k], found)
    return found


def make_kernel(n_vocab, n_tok, rows, depth, columns, tokens, share, seqs):
    na = n_tok // 4
    n_dev = n_vocab * n_tok
    secs = sections_of(columns)
    n_sec = len(secs)
    half = rows // HALVES
    per_tile = LANES // share
    pairs = rows * 2
    steps_of = [(1, 0), (0, 1)] if na > 2 else [(0, 1)]
    for i in range(2, na - 1):
        steps_of += [(i, 0), (i - 1, 1)]
    if na > 2:
        steps_of += [(na - 2, 1)]
    n_step = 3 + len(steps_of)
    step_at = {item: 3 + k for k, item in enumerate(steps_of)}
    step_at[(0, 0)] = 2

    def z_time(d, h):
        return [(2, 3), (5, 6), (9, 10)][d - 1][h] if d <= 3 else 3 * (2 * d - 3) + h

    def kernel(hidden, gain, weights, ids, mask, seq, adv, prox, behav,
               logp_out, loss_out, policy_out, means_out,
               x, w, logits, m_ref, s_ref, p_ref, t_ref, stats, got, tile, tiles,
               w_sem, recv, send, st_send, st_recv, ls_send, ls_recv):
        v = lax.axis_index("vocab")
        t = lax.axis_index("tok")
        me = v * n_tok + t
        c = t % 2
        b = (t // 2) % 2
        a = t // 4
        plane = v % 2
        active = c == plane
        passive = c != plane

        loads = [pltpu.make_async_copy(weights.at[:, pl.ds(lo, n)], w[k], w_sem.at[k])
                 for k, (lo, n) in enumerate(secs)]
        for load in loads:
            load.start()
        barrier = pltpu.get_barrier_semaphore()

        @pl.loop(0, n_dev)
        def _(other):
            @pl.when(other != me)
            def _():
                pl.semaphore_signal(barrier, inc=1, device_id=(other // n_tok, other % n_tok), device_id_type=MESH)

        @pl.loop(0, rows // 16)
        def _(r):
            at = pl.ds(pl.multiple_of(r * 16, 16), 16)
            values = hidden[at, :].astype(jnp.float32)
            scale = lax.rsqrt(jnp.mean(values * values, axis=1, keepdims=True) + 1e-06)
            x[t, at, :] = (values * scale * gain[...]).astype(jnp.bfloat16)

        for k in range(n_sec):
            logits[k][...] = jnp.zeros_like(logits[k])
        m_ref[...] = jnp.full_like(m_ref, LOW)
        s_ref[...] = jnp.zeros_like(s_ref)
        p_ref[...] = jnp.zeros_like(p_ref)
        t_ref[...] = jnp.full_like(t_ref, -1)
        stats[...] = jnp.zeros_like(stats)
        pl.semaphore_wait(barrier, n_dev - 1)

        def slot_of(sa, sb, sc):
            return sa * 4 + sb * 2 + sc

        def other_row(i):
            up = i + jnp.where(i >= a, 1, 0)
            mirror = na - 1 - a
            down = na - 1 - (i + jnp.where(i >= mirror, 1, 0))
            return jnp.where(a * 2 < na, up, down)

        def piece(slot, h, way, dv, dt):
            ref = x.at[slot, pl.ds(h * half, half), :]
            return pltpu.make_async_remote_copy(
                src_ref=ref, dst_ref=ref, send_sem=send.at[way, slot, h], recv_sem=recv.at[slot, h],
                device_id=(dv, dt), device_id_type=MESH)

        closing = []

        def ship(when, pred, slot, h, way, dv, dt):
            @pl.when(pred if when is None else jnp.logical_and(when, pred))
            def _():
                copy = piece(slot, h, way, dv, dt)
                if closing:
                    copy.wait_send()
                else:
                    copy.start()

        def take(when, pred, slot, h):
            if not closing:
                @pl.when(jnp.logical_and(when, pred))
                def _():
                    piece(slot, h, 0, v, t + 1 - 2 * c).wait_recv()

        flip_v = v + 1 - 2 * plane
        mate = t + 1 - 2 * c
        beside = slot_of(a, 1 - b, c)
        events = {}

        def on(q, fn):
            events.setdefault(q, []).append(fn)

        def to_mate(when, pred, slot, h):
            ship(when, pred, slot, h, 4, v, mate)

        def own_x(pred):
            def fn(when):
                for h in range(HALVES):
                    ship(when, pred, t, h, 2, v, beside)
            return fn

        on(3, own_x(passive))

        def z_take(d, h):
            def fn(when):
                for side in (-1, 1):
                    far = a + side * d
                    there = jnp.logical_and(far >= 0, far < na)
                    pred = jnp.logical_and(active, there)
                    slot = slot_of(jnp.clip(far, 0, na - 1), b, c)

                    take(when, pred, slot, h)
                    nxt = a - side
                    go = jnp.logical_and(pred, jnp.logical_and(nxt >= 0, nxt < na))
                    ship(when, go, slot, h, 0 if side > 0 else 1, v, slot_of(jnp.clip(nxt, 0, na - 1), b, c))
                    to_mate(when, pred, slot, h)
            return fn

        def beside_take(pred, h):
            def fn(when):
                take(when, pred, beside, h)
                to_mate(when, pred, beside, h)
            return fn

        def x_send(i, h):
            return lambda when: ship(when, active, slot_of(other_row(i), b, c), h, 2, v, beside)

        def y_send(i, e, h):
            return lambda when: ship(when, active, slot_of(other_row(i), b if e == 0 else 1 - b, c), h, 3, flip_v, t)

        def x_take(i, h):
            def fn(when):
                slot = slot_of(other_row(i), 1 - b, c)
                take(when, active, slot, h)
                to_mate(when, active, slot, h)
            return fn

        def y_take(i, e, h):
            def fn(when):
                slot = slot_of(other_row(i), b if e == 0 else 1 - b, c)
                take(when, passive, slot, h)
                to_mate(when, passive, slot, h)
            return fn

        for h in range(HALVES):
            on(2 + h, beside_take(active, h))
            on(5 + h, beside_take(passive, h))
        for d in range(1, na):
            for h in range(HALVES):
                on(z_time(d, h), z_take(d, h))
        for i in range(na - 1):
            for h in range(HALVES):
                zt = z_time(i + 1, h)
                on(max(zt, 5), x_send(i, h))
                on(zt, y_send(i, 0, h))
                xt = 3 * step_at[(i, 1)] - (4 if i == 0 else 7) + h
                on(xt, x_take(i, h))
                on(xt, y_send(i, 1, h))
                for e in (0, 1):
                    yt = 3 * step_at[(i, e)] - (1 - h)
                    if (i, e) == (0, 0):
                        yt = (4, 6)[h]
                    on(yt, y_take(i, e, h))

        def open_sends():
            for h in range(HALVES):
                to_mate(None, me >= 0, t, h)
                for side in (-1, 1):
                    nxt = a - side
                    go = jnp.logical_and(active, jnp.logical_and(nxt >= 0, nxt < na))
                    ship(None, go, t, h, 0 if side > 0 else 1, v, slot_of(jnp.clip(nxt, 0, na - 1), b, c))
            own_x(active)(None)

        open_sends()

        def slots_at(s):
            first = [slot_of(a, b, 0), slot_of(a, 1 - b, plane), slot_of(a, 1 - b, 1 - plane)]
            second = [slot_of(a, b, 1), slot_of(other_row(0), b, plane), slot_of(other_row(0), b, 1 - plane)]
            for i, e in steps_of:
                sb = b if e == 0 else 1 - b
                first.append(slot_of(other_row(i), sb, 0))
                second.append(slot_of(other_row(i), sb, 1))
            return pick(s, first), pick(s, second)

        first_col = me * columns
        lane = lax.broadcasted_iota(jnp.int32, (LANES, LANES), 1)
        group = 64

        def absorb(k):
            lo, n = secs[k]
            count = padded(n) // LANES
            ref = logits[k]
            lanes = lax.broadcasted_iota(jnp.int32, (group, LANES), 1)
            for r in range(0, pairs, group):
                at = slice(r, r + group)

                def value(j):
                    found = ref[at, j * LANES:(j + 1) * LANES]
                    left = n - j * LANES
                    return found if left >= LANES else jnp.where(lanes < left, found, LOW)
                old = m_ref[at, :]
                new = old
                chosen = p_ref[at, :]
                where = t_ref[at, :]
                for j in range(count):
                    item = value(j)
                    new = jnp.maximum(new, item)
                    hit = where == lo + j * LANES
                    if n - j * LANES < LANES:
                        hit = jnp.logical_and(hit, lanes < n - j * LANES)
                    chosen = jnp.where(hit, item, chosen)
                total = s_ref[at, :] * jnp.exp(old - new)
                for j in range(count):
                    total = total + jnp.exp(value(j) - new)
                m_ref[at, :] = new
                s_ref[at, :] = total
                p_ref[at, :] = chosen

        def stat_copy(slot, o):
            return pltpu.make_async_remote_copy(
                src_ref=stats.at[slot], dst_ref=got.at[me], send_sem=st_send.at[o], recv_sem=st_recv.at[me],
                device_id=(o // n_tok, o % n_tok), device_id_type=MESH)

        def settle(s):
            for k, slot in enumerate(slots_at(s)):
                at = slice(k * rows, (k + 1) * rows)
                m = m_ref[at, :].T
                top = jnp.max(m, axis=0, keepdims=True)
                total = jnp.sum(s_ref[at, :].T * jnp.exp(m - top), axis=0, keepdims=True)
                chosen = jnp.sum(p_ref[at, :].T, axis=0, keepdims=True)
                stats[slot, 0:1, :] = top
                stats[slot, 1:2, :] = total
                stats[slot, 2:3, :] = chosen
            for k, slot in enumerate(slots_at(s)):
                for g in range(per_tile):
                    o = slot * per_tile + g

                    @pl.when(o != me)
                    def _():
                        stat_copy(slot, o).start()

        def begin(s):
            for k, slot in enumerate(slots_at(s)):
                at = slice(k * rows, (k + 1) * rows)
                line = jnp.broadcast_to(ids[pl.ds(slot, 1), :], (LANES, LANES))
                t_ref[at, :] = line.T - first_col - lane
            m_ref[...] = jnp.full_like(m_ref, LOW)
            s_ref[...] = jnp.zeros_like(s_ref)
            p_ref[...] = jnp.zeros_like(p_ref)

        def run_step(s, carry):
            one, two = slots_at(s)
            for point in range(3):
                for q in sorted(events):
                    if q % 3 == point:
                        when = s == q // 3
                        for fn in events[q]:
                            fn(when)
                if point == 0:
                    for slot in (one, two):
                        for h in range(HALVES):
                            take(s >= 0, slot % 2 != c, slot, h)
                if point < n_sec:
                    @pl.when(s == 0)
                    def _():
                        loads[point].wait()
                    lo, n = secs[point]
                    block = jnp.concatenate([x[one], x[two]], axis=0)
                    logits[point][:, 0:n] = jnp.dot(block, w[point][...], preferred_element_type=jnp.float32)
                    absorb((point - 1) % n_sec)
                    if point == 0:
                        @pl.when(s > 0)
                        def _():
                            settle(s - 1)
                        begin(s)
            return carry

        lax.fori_loop(0, n_step, run_step, 0)
        absorb(n_sec - 1)
        settle(n_step - 1)

        mine = me // per_tile
        got[me, :, :] = stats[mine]

        @pl.loop(0, n_dev)
        def _(o):
            @pl.when(o != me)
            def _():
                pltpu.make_async_remote_copy(
                    src_ref=stats.at[mine], dst_ref=got.at[o], send_sem=st_send.at[o], recv_sem=st_recv.at[o],
                    device_id=(o // n_tok, o % n_tok), device_id_type=MESH).wait_recv()

        peak = jnp.full((8, LANES), LOW, jnp.float32)
        for o in range(n_dev):
            peak = jnp.maximum(peak, got[o])
        peak = peak[0:1, :]
        total = jnp.zeros((1, LANES), jnp.float32)
        chosen = jnp.zeros((1, LANES), jnp.float32)
        for o in range(n_dev):
            total = total + got[o, 1:2, :] * jnp.exp(got[o, 0:1, :] - peak)
            chosen = chosen + got[o, 2:3, :]
        wide = chosen - peak - jnp.log(total)
        logp = wide[:, 0:share]
        for g in range(1, per_tile):
            logp = jnp.where(me % per_tile == g, wide[:, g * share:(g + 1) * share], logp)
        prox_v = prox[...]
        adv_v = adv[...]
        weight_b = jnp.minimum(jnp.exp(prox_v - behav[...]), 5.0)
        ratio = jnp.exp(logp - prox_v)
        surr = jnp.minimum(ratio * adv_v, jnp.clip(ratio, 0.8, 1.2) * adv_v)
        surr = jnp.where(adv_v < 0, jnp.maximum(surr, 3.0 * adv_v), surr)
        token_loss = -weight_b * surr
        logp_out[...] = logp
        loss_out[...] = token_loss
        live = mask[...].astype(jnp.float32)
        tile[...] = jnp.zeros_like(tile)
        for i in range(seqs):
            member = jnp.where(seq[...] == i, live, 0.0)
            for k, part in enumerate((member * token_loss, member * (logp - prox_v), member)):
                tile[k * seqs + i:k * seqs + i + 1, 0:share] = part
        tiles[me, :, :] = tile[...]

        def loss_copy(o, where):
            return pltpu.make_async_remote_copy(
                src_ref=tile, dst_ref=tiles.at[where], send_sem=ls_send.at[o], recv_sem=ls_recv.at[where],
                device_id=(o // n_tok, o % n_tok), device_id_type=MESH)

        @pl.loop(0, n_dev)
        def _(o):
            @pl.when(o != me)
            def _():
                loss_copy(o, me).start()

        closing.append(True)
        open_sends()
        for q in sorted(events):
            for fn in events[q]:
                fn(None)

        @pl.loop(0, n_dev)
        def _(o):
            @pl.when(o != me)
            def _():
                stat_copy(o // per_tile, o).wait_send()
                loss_copy(o, o).wait()

        summed = tiles[0]
        for o in range(1, n_dev):
            summed = summed + tiles[o]
        sums = jnp.sum(summed, axis=1, keepdims=True)
        loss_sum, diff_sum, count = (sums[k * seqs:(k + 1) * seqs] for k in range(3))
        policy_out[...] = jnp.sum(loss_sum, axis=0, keepdims=True) / jnp.maximum(jnp.sum(count, axis=0, keepdims=True), 1.0)
        floor = jnp.maximum(count, 1.0)
        means_out[:, 0:1] = loss_sum / floor
        means_out[:, 1:2] = diff_sum / floor

    tile_rows = (3 * seqs + 7) // 8 * 8
    scratch = [
        pltpu.VMEM((n_tok, rows, depth), jnp.bfloat16),
        [pltpu.VMEM((depth, n), jnp.bfloat16) for _, n in secs],
        [pltpu.VMEM((pairs, padded(n)), jnp.float32) for _, n in secs],
        pltpu.VMEM((pairs, LANES), jnp.float32),
        pltpu.VMEM((pairs, LANES), jnp.float32),
        pltpu.VMEM((pairs, LANES), jnp.float32),
        pltpu.VMEM((pairs, LANES), jnp.int32),
        pltpu.VMEM((n_tok, 8, LANES), jnp.float32),
        pltpu.VMEM((n_dev, 8, LANES), jnp.float32),
        pltpu.VMEM((tile_rows, LANES), jnp.float32),
        pltpu.VMEM((n_dev, tile_rows, LANES), jnp.float32),
        pltpu.SemaphoreType.DMA((n_sec,)),
        pltpu.SemaphoreType.DMA((n_tok, HALVES)),
        pltpu.SemaphoreType.DMA((5, n_tok, HALVES)),
        pltpu.SemaphoreType.DMA((n_dev,)),
        pltpu.SemaphoreType.DMA((n_dev,)),
        pltpu.SemaphoreType.DMA((n_dev,)),
        pltpu.SemaphoreType.DMA((n_dev,)),
    ]
    return kernel, scratch


def solution(mesh):
    n_vocab, n_tok = mesh.shape["vocab"], mesh.shape["tok"]

    def shards(hidden, norm_gain, unembed, target_ids, loss_mask, seq_ids, advantages, prox_logp, behav_logp):
        rows, depth = hidden.shape
        columns = unembed.shape[1]
        tokens = target_ids.shape[0]
        share = loss_mask.shape[0]
        seqs = tokens // LENGTH
        kernel, scratch = make_kernel(n_vocab, n_tok, rows, depth, columns, tokens, share, seqs)
        vmem = pl.BlockSpec(memory_space=pltpu.VMEM)
        logp, token_loss, policy, means = pl.pallas_call(
            kernel,
            out_shape=(
                jax.ShapeDtypeStruct((1, share), jnp.float32),
                jax.ShapeDtypeStruct((1, share), jnp.float32),
                jax.ShapeDtypeStruct((1, 1), jnp.float32),
                jax.ShapeDtypeStruct((seqs, 2), jnp.float32),
            ),
            in_specs=[vmem, vmem, pl.BlockSpec(memory_space=pl.ANY)] + [vmem] * 6,
            out_specs=(vmem,) * 4,
            scratch_shapes=scratch,
            compiler_params=pltpu.CompilerParams(collective_id=0, has_side_effects=True, vmem_limit_bytes=67043328),
        )(
            hidden, norm_gain.reshape(1, depth), unembed, target_ids.reshape(n_tok, rows),
            *(item.reshape(1, share) for item in (loss_mask, seq_ids, advantages, prox_logp, behav_logp)),
        )
        return logp.reshape(share), token_loss.reshape(share), policy.reshape(()), means.T

    both = P(("vocab", "tok"))
    in_specs = (P("tok", None), P(), P(None, ("vocab", "tok")), P(), both, both, both, both, both)
    return jax.shard_map(shards, mesh=mesh, in_specs=in_specs, out_specs=(both, both, P(), P()), check_vma=False)
```
